32 devices in a mesh: section: 2 (over core), node: 4 (over z), local: 4 (over y, x).
Axes of the slice: x: 2, y: 2, z: 4, core: 2. Of those that a mesh axis runs over, the one named last changes fastest.
Arguments:
- tokens: bfloat16 [2, 1024, 768], P(None, ('node', 'local')), may hold values from -18 to 18
- expert_ids: int32 [2, 2, 1024, 2], P('section', None, ('node', 'local')), may hold values from 0 to 15, as said below
- slots: int32 [2, 2, 1024, 2], P('section', None, ('node', 'local')), may hold values from -1 to 31, as said below
- gates: float32 [2, 2, 1024, 2], P('section', None, ('node', 'local')), may hold values from 0.2 to 1
- gain: float32 [2, 768], P('section'), may hold values from 0.5 to 1.5
- w_gate: bfloat16 [2, 16, 768, 3072], P('section', ('node', 'local')), may hold values from -0.21875 to 0.21875
- w_up: bfloat16 [2, 16, 768, 3072], P('section', ('node', 'local')), may hold values from -0.21875 to 0.21875
- w_down: bfloat16 [2, 16, 3072, 768], P('section', ('node', 'local')), may hold values from -0.109375 to 0.109375
Outputs:
- hidden: bfloat16 [2, 2, 1024, 768], P('section', None, ('node', 'local'))
The draws below stay inside these ranges and needn't reach their ends.
Inputs may be any that keep to these rules, and one draw needn't show every extreme that they name: `expert_ids`: in each layer and micro-batch the two ids of a token differ, no expert is named by more than 256 tokens, and some expert is named by exactly 256. Expert e lies on node e // 4. Among one device's 64 tokens of a micro-batch and layer, the kept tokens that reach one node hold distinct slots below 32, and the two choices of a token on one node carry the same slot; -1 marks a dropped choice.
All inputs are finite; a program needn't handle non-finite values.
Results may differ from the reference program's by a relative error of at most 0.0085.
Values may be sent and summed in bfloat16 or wider, within the bound.
A program may use at most 64 MiB of HBM per device.

```python
import math
import jax
import jax.numpy as jnp
from jax import lax

D = 768
FF = 3072
TOP = 2
TOK_MB = 64
MICRO = 2
LAYERS = 2
EXPERTS = 16
TOKENS = 1024
CAP = 32
ECAP = 256
N_NODE = 4
N_LOCAL = 4


def one_group(group_key):
    subkeys = jax.random.split(group_key, 5)
    node_order = jax.random.permutation(subkeys[0], N_NODE)
    local_order = jax.random.permutation(subkeys[1], N_LOCAL)
    second_node_order = jax.random.permutation(subkeys[4], N_NODE)
    half_count = EXPERTS // 2
    quarter = EXPERTS // 4
    half_local = N_LOCAL // 2
    mean_load = 2 * TOK_MB
    rank_ids = jnp.arange(half_count, dtype=jnp.int32)
    upper_gain = mean_load * (quarter - rank_ids) // quarter
    lower_gain = mean_load * (quarter - (half_count - 1 - rank_ids)) // quarter
    quotas = jnp.where(rank_ids < quarter, mean_load + upper_gain, mean_load - lower_gain)
    bounds = jnp.cumsum(quotas)
    places = jnp.arange(TOKENS, dtype=jnp.int32)
    which_rank = jnp.sum((places[:, None] >= bounds[None, :]).astype(jnp.int32), axis=1)
    first_node = node_order[which_rank // half_local]
    second_node = second_node_order[which_rank // half_local]
    first_ids = first_node * N_LOCAL + local_order[which_rank % half_local]
    second = second_node * N_LOCAL + local_order[half_local + which_rank % half_local]
    first_ids = first_ids[jax.random.permutation(subkeys[2], TOKENS)]
    second = second[jax.random.permutation(subkeys[3], TOKENS)]
    routing = jnp.stack([first_ids, second], axis=1).astype(jnp.int32)
    device_route = routing.reshape(N_NODE * N_LOCAL, TOK_MB, 2)
    node_route = device_route // N_LOCAL
    node_span = jnp.arange(N_NODE, dtype=jnp.int32)
    touched = ((node_route[..., 0:1] == node_span) | (node_route[..., 1:2] == node_span)).astype(jnp.int32)
    before = jnp.cumsum(touched, axis=1) - touched
    slot_pick = jnp.take_along_axis(before, node_route, axis=2)
    slot_vals = jnp.where(slot_pick < CAP, slot_pick, -1).reshape(TOKENS, 2).astype(jnp.int32)
    return (routing, slot_vals)


def route_tables(key):
    base_key = jax.random.fold_in(key, 7)
    group_keys = jax.random.split(base_key, LAYERS * MICRO)
    expert_table, slot_table = jax.vmap(one_group)(group_keys)
    return (expert_table.reshape(LAYERS, MICRO, TOKENS, 2), slot_table.reshape(LAYERS, MICRO, TOKENS, 2))


def draw_expert_ids(key, part):
    return route_tables(key)[0]


def draw_slots(key, part):
    return route_tables(key)[1]


def draw_tokens(key, part):
    subkeys = jax.random.split(jax.random.fold_in(key, 3), 2)
    values = jnp.clip(jax.random.normal(subkeys[0], (MICRO, TOKENS, D), jnp.float32), -6.0, 6.0)
    scales = jnp.exp(jax.random.uniform(subkeys[1], (MICRO, TOKENS, 1), jnp.float32, math.log(0.5), math.log(2.0)))
    return (values * scales).astype(jnp.bfloat16)


def steps_of(key, shape, cuts, low, high):
    level = 1.0
    for dim, shards_of in cuts:
        draws = jax.random.uniform(jax.random.fold_in(jax.random.fold_in(key, 6), dim), (shards_of,), jnp.float32, low / len(cuts), high / len(cuts))
        level = level * jnp.repeat(jnp.exp(draws), shape[dim] // shards_of).reshape((-1,) + (1,) * (len(shape) - 1 - dim))
    return level


def centred(own_key, dims, deviation, most, pieces=(), kind=jnp.bfloat16):
    result = jax.random.normal(own_key, dims, jnp.float32) * deviation
    if len(pieces) > 0:
        result = steps_of(own_key, dims, pieces, -0.22, 0.18) * result
    return jnp.clip(result, min=-most, max=most).astype(kind)


def setup_inputs(seed: int = 0) -> dict:
    key_list = jax.random.split(jax.random.key(seed), 9)
    tokens = draw_tokens(jax.random.fold_in(key_list[8], 71), 0)
    expert_ids = draw_expert_ids(jax.random.fold_in(key_list[8], 71), 0)
    slots = draw_slots(jax.random.fold_in(key_list[8], 71), 0)
    gates = jnp.clip(0.2 + 0.8 * jax.random.uniform(key_list[3], (LAYERS, MICRO, TOKENS, TOP), jnp.float32) ** steps_of(key_list[3], (LAYERS, MICRO, TOKENS, TOP), ((0, 2), (2, 16)), -0.2, 0.2), 0.2, 1.0)
    gain = jnp.clip(1.0 + 0.1 * jax.random.normal(key_list[4], (LAYERS, D), jnp.float32), 0.5, 1.5)
    w_gate = centred(key_list[5], (LAYERS, EXPERTS, D, FF), D ** -0.5, 0.21875, ((0, 2), (1, 16)))
    w_up = centred(key_list[6], (LAYERS, EXPERTS, D, FF), D ** -0.5, 0.21875, ((0, 2), (1, 16)))
    w_down = centred(key_list[7], (LAYERS, EXPERTS, FF, D), FF ** -0.5, 0.109375, ((0, 2), (1, 16)))
    return {"tokens": tokens, "expert_ids": expert_ids, "slots": slots, "gates": gates, "gain": gain, "w_gate": w_gate, "w_up": w_up, "w_down": w_down}


def rms_normed(values, gain_row):
    floats = values.astype(jnp.float32)
    mean_square = lax.optimization_barrier(jnp.mean(floats * floats, axis=-1, keepdims=True))
    return (floats * lax.rsqrt(mean_square + 1e-05) * gain_row).astype(jnp.bfloat16)

def expert_apply(picked, gate_mat, up_mat, down_mat):
    gate_act = jnp.dot(picked, gate_mat, preferred_element_type=jnp.float32)
    up_act = jnp.dot(picked, up_mat, preferred_element_type=jnp.float32)
    inner = (jax.nn.gelu(gate_act, approximate=True) * up_act).astype(jnp.bfloat16)
    return jnp.dot(inner, down_mat, preferred_element_type=jnp.float32)

def moe_layer(layer_in, routing, slot_ids, gate_vals, gain_row, gate_all, up_all, down_all):
    normed = rms_normed(layer_in, gain_row)
    keep_weight = jnp.where(slot_ids >= 0, gate_vals, jnp.float32(0.0)).astype(jnp.float32)

    def per_expert(totals, expert):
        hit_mask = routing == expert
        any_hit = jnp.any(hit_mask, axis=1)
        row_index = jnp.nonzero(any_hit, size=ECAP, fill_value=0)[0].astype(jnp.int32)
        valid_rows = jnp.arange(ECAP, dtype=jnp.int32) < jnp.sum(any_hit.astype(jnp.int32))
        picked = normed[row_index]
        outputs = expert_apply(picked, gate_all[expert], up_all[expert], down_all[expert])
        row_weight = lax.optimization_barrier(jnp.sum(jnp.where(hit_mask, keep_weight, jnp.float32(0.0)), axis=1))[row_index]
        row_weight = jnp.where(valid_rows, row_weight, jnp.float32(0.0))
        scaled = lax.optimization_barrier((row_weight[:, None] * outputs).astype(jnp.bfloat16)).astype(jnp.float32)
        choice_mask = (hit_mask[row_index] & valid_rows[:, None]).astype(jnp.float32)
        totals = totals.at[row_index].add(scaled[:, None, :] * choice_mask[:, :, None])
        return (totals, None)
    start = jnp.zeros((layer_in.shape[0], 2, layer_in.shape[1]), jnp.float32)
    totals, _ = lax.scan(per_expert, start, jnp.arange(EXPERTS, dtype=jnp.int32))
    same_node = routing[:, 0] // N_LOCAL == routing[:, 1] // N_LOCAL
    pair_sum = totals[:, 0] + totals[:, 1]
    together = lax.optimization_barrier(pair_sum.astype(jnp.bfloat16)).astype(jnp.float32)
    mixed_rows = jnp.where(same_node[:, None], together, pair_sum)
    return (layer_in.astype(jnp.float32) + mixed_rows).astype(jnp.bfloat16)

def reference(tokens, expert_ids, slots, gates, gain, w_gate, w_up, w_down):
    current = [tokens[batch_index] for batch_index in range(MICRO)]
    stacked = []
    for layer_index in range(LAYERS):
        produced = []
        for batch_index in range(MICRO):
            produced.append(moe_layer(current[batch_index], expert_ids[layer_index, batch_index], slots[layer_index, batch_index], gates[layer_index, batch_index], gain[layer_index], w_gate[layer_index], w_up[layer_index], w_down[layer_index]))
        stacked.append(jnp.stack(produced))
        current = produced
    return jnp.stack(stacked)
```

```python
import functools

import jax
import jax.numpy as jnp
from jax import lax
from jax.experimental import pallas as pl
from jax.experimental.pallas import tpu as pltpu
from jax.sharding import PartitionSpec as P

MESH = pl.DeviceIdType.MESH
LANES = 128
FF_CHUNKS = 3


def over_rows(a, b, precision=None):
    return lax.dot_general(
        a, b, (((0,), (0,)), ((), ())), precision=precision, preferred_element_type=jnp.float32
    )


def relay_kernel(
    sizes,
    tok_ref, ids_ref, slots_ref, gates_ref, gain_ref, wg_hbm, wu_hbm, wd_hbm,
    out_ref,
    held, packed, arrived, answer, returned, hits, meta_out, meta_in, pick, pick_w, acc,
    wg, wu, wd,
    w_sem, meta_send, meta_recv, d_send, d_recv, r_send, r_recv, relay_send, relay_recv,
):
    n_sec, n_node, n_local, micro, toks, width, cap, limit = sizes
    n = n_node * n_local
    total = n * cap
    groups = total // LANES
    sec = lax.axis_index("section")
    node = lax.axis_index("node")
    local = lax.axis_index("local")
    me = node * n_local + local

    def device(p):
        return {"node": lax.div(p, n_local), "local": lax.rem(p, n_local)}

    def peers(body):
        lax.fori_loop(1, n, lambda i, c: (body(lax.rem(me + i, n)), c)[1], 0)

    barrier = pltpu.get_barrier_semaphore()
    peers(lambda p: pl.semaphore_signal(barrier, inc=1, device_id=device(p), device_id_type=MESH))
    for i in range(1, n_sec):
        pl.semaphore_signal(
            barrier, inc=1, device_id={"section": lax.rem(sec + i, n_sec)}, device_id_type=MESH
        )

    def weight_copies(c):
        chunk = wg.shape[2]
        cols = pl.ds(pl.multiple_of(c * chunk, chunk), chunk)
        return (
            pltpu.make_async_copy(wg_hbm.at[:, cols], wg.at[c], w_sem.at[0, c]),
            pltpu.make_async_copy(wu_hbm.at[:, cols], wu.at[c], w_sem.at[1, c]),
            pltpu.make_async_copy(wd_hbm.at[cols, :], wd.at[c], w_sem.at[2, c]),
        )

    for c in range(FF_CHUNKS):
        for copy in weight_copies(c):
            copy.start()

    def meta_copy(p):
        return pltpu.make_async_remote_copy(
            meta_out.at[p], meta_in.at[me], meta_send.at[p], meta_recv.at[me],
            device_id=device(p), device_id_type=MESH,
        )

    def out_copy(mb, p):
        return pltpu.make_async_remote_copy(
            packed.at[mb, lax.div(p, n_local)], arrived.at[mb, me], d_send.at[mb, p],
            d_recv.at[mb, me], device_id=device(p), device_id_type=MESH,
        )

    def back_copy(mb, p):
        return pltpu.make_async_remote_copy(
            answer.at[mb, p], returned.at[mb, me], r_send.at[mb, p],
            r_recv.at[mb, me], device_id=device(p), device_id_type=MESH,
        )

    def arrival(buffer, sem, p):
        return pltpu.make_async_remote_copy(
            buffer.at[p], buffer.at[p], sem.at[p], sem.at[p],
            device_id=device(p), device_id_type=MESH,
        )

    def relay_copy(mb):
        return pltpu.make_async_remote_copy(
            out_ref.at[mb], held.at[mb], relay_send.at[mb], relay_recv.at[mb],
            device_id={"section": lax.rem(sec + 1, n_sec)}, device_id_type=MESH,
        )

    slot_span = lax.broadcasted_iota(jnp.int32, (toks, n_node * cap), 1)
    exp_span = lax.broadcasted_iota(jnp.int32, (toks, n), 1)
    lane_span = lax.broadcasted_iota(jnp.int32, (toks, LANES), 1)
    row_span = lax.broadcasted_iota(jnp.int32, (n, micro * groups, LANES), 1)
    my_group = lax.div(me * cap, LANES)
    my_lane = lax.rem(me * cap, LANES)
    meta = jnp.zeros((n, micro * groups, LANES), jnp.float32)
    for mb in range(micro):
        hit = None
        weights = None
        for k in range(2):
            e = ids_ref[mb, :, k : k + 1]
            s = slots_ref[mb, :, k : k + 1]
            g = gates_ref[mb, :, k : k + 1]
            pos = jnp.where(s >= 0, lax.div(e, jnp.full_like(e, n_local)) * cap + s, -1)
            this = jnp.where(pos == slot_span, 1.0, 0.0)
            hit = this if hit is None else jnp.maximum(hit, this)
            lane = jnp.where(s >= 0, my_lane + s, -1)
            part = over_rows(
                jnp.where(e == exp_span, g, 0.0),
                jnp.where(lane == lane_span, 1.0, 0.0),
                lax.Precision.HIGHEST,
            )
            weights = part if weights is None else weights + part
        hits[mb] = hit.astype(jnp.bfloat16)
        meta = meta + jnp.where(row_span == mb * groups + my_group, weights[:, None, :], 0.0)
    meta_out[...] = meta
    meta_in[me] = meta_out[me]

    def pack(mb, h):
        floats = h.astype(jnp.float32)
        mean_square = jnp.mean(floats * floats, axis=-1, keepdims=True)
        normed = (floats * lax.rsqrt(mean_square + 1e-05) * gain_ref[...]).astype(jnp.bfloat16)
        rows = over_rows(hits[mb], normed)
        for j in range(n_node):
            packed[mb, j] = rows[j * cap : (j + 1) * cap].astype(jnp.bfloat16)
        arrived[mb, me] = packed[mb, node]

    @pl.when(sec == 0)
    def _():
        held[...] = tok_ref[...]
        pack(0, held[0])

    pl.semaphore_wait(barrier, n - 1 + n_sec - 1)
    peers(lambda p: meta_copy(p).start())

    @pl.when(sec == 0)
    def _():
        peers(lambda p: out_copy(0, p).start())
        for mb in range(1, micro):
            pack(mb, held[mb])
            peers(lambda p: out_copy(mb, p).start())

    peers(lambda p: arrival(meta_in, meta_recv, p).wait_recv())
    meta = jnp.sum(meta_in[...], axis=0)
    upto = lax.broadcasted_iota(jnp.int32, (total, total), 0) <= lax.broadcasted_iota(
        jnp.int32, (total, total), 1
    )
    upto = jnp.where(upto, 1.0, 0.0).astype(jnp.bfloat16)
    spot = lax.broadcasted_iota(jnp.int32, (limit, total), 0).astype(jnp.float32)
    for mb in range(micro):
        w_row = jnp.concatenate(
            [meta[mb * groups + g : mb * groups + g + 1] for g in range(groups)], axis=1
        )
        w_rows = jnp.broadcast_to(w_row, (8, total))
        chosen = jnp.where(w_rows > 0.0, 1.0, 0.0)
        rank = jnp.dot(chosen.astype(jnp.bfloat16), upto, preferred_element_type=jnp.float32)
        rank = jnp.where(w_rows > 0.0, rank - 1.0, -1.0)
        is_at = spot == jnp.broadcast_to(rank[0:1], (limit, total))
        pick[mb] = jnp.where(is_at, 1.0, 0.0).astype(jnp.bfloat16)
        pick_w[mb] = jnp.sum(
            jnp.where(is_at, jnp.broadcast_to(w_row, (limit, total)), 0.0), axis=1, keepdims=True
        )

    @pl.when(sec > 0)
    def _():
        for mb in range(micro):
            relay_copy(mb).wait_recv()
            pack(mb, held[mb])
            peers(lambda p: out_copy(mb, p).start())

    def flat(blocks):
        if cap % 16:
            return blocks.astype(jnp.float32).reshape(total, width).astype(jnp.bfloat16)
        return blocks.reshape(total, width)

    for mb in range(micro):
        peers(lambda p: arrival(arrived.at[mb], d_recv.at[mb], p).wait_recv())
        rows = flat(arrived[mb])
        x = jnp.dot(pick[mb], rows, preferred_element_type=jnp.float32).astype(jnp.bfloat16)
        acc[...] = jnp.zeros_like(acc)

        def chunk_step(c, carry):
            if mb == 0:
                for copy in weight_copies(c):
                    copy.wait()
            gate = jnp.dot(x, wg[c], preferred_element_type=jnp.float32)
            up = jnp.dot(x, wu[c], preferred_element_type=jnp.float32)
            inner = (jax.nn.gelu(gate, approximate=True) * up).astype(jnp.bfloat16)
            acc[...] += jnp.dot(inner, wd[c], preferred_element_type=jnp.float32)
            return carry

        lax.fori_loop(0, FF_CHUNKS, chunk_step, 0)
        scaled = (pick_w[mb] * acc[...]).astype(jnp.bfloat16)
        spread = over_rows(pick[mb], scaled)
        answer[mb] = spread.reshape(n, cap, width).astype(jnp.bfloat16)
        returned[mb, me] = answer[mb, me]
        peers(lambda p: back_copy(mb, p).start())

    for mb in range(micro):
        peers(lambda p: arrival(returned.at[mb], r_recv.at[mb], p).wait_recv())
        sums = []
        for j in range(n_node):
            block = returned[mb, j * n_local].astype(jnp.float32)
            for i in range(1, n_local):
                block = block + returned[mb, j * n_local + i].astype(jnp.float32)
            sums.append(block)
        combined = jnp.concatenate(sums, axis=0).astype(jnp.bfloat16)
        mixed = jnp.dot(hits[mb], combined, preferred_element_type=jnp.float32)
        out_ref[mb] = (held[mb].astype(jnp.float32) + mixed).astype(jnp.bfloat16)

        @pl.when(sec < n_sec - 1)
        def _():
            relay_copy(mb).start()

    def settle(p):
        meta_copy(p).wait_send()
        for mb in range(micro):
            out_copy(mb, p).wait_send()
            back_copy(mb, p).wait_send()

    peers(settle)

    @pl.when(sec < n_sec - 1)
    def _():
        for mb in range(micro):
            relay_copy(mb).wait_send()


def solution(mesh):
    n_sec, n_node, n_local = mesh.shape["section"], mesh.shape["node"], mesh.shape["local"]
    n = n_node * n_local

    def on_device(tokens, expert_ids, slots, gates, gain, w_gate, w_up, w_down):
        micro, toks, width = tokens.shape
        hidden = w_gate.shape[3]
        cap = 2 * toks // n_node
        limit = 4 * toks
        total = n * cap
        chunk = hidden // FF_CHUNKS
        sizes = (n_sec, n_node, n_local, micro, toks, width, cap, limit)
        half, full = jnp.bfloat16, jnp.float32
        vmem = pl.BlockSpec(memory_space=pltpu.VMEM)
        hbm = pl.BlockSpec(memory_space=pl.ANY)
        dma = pltpu.SemaphoreType.DMA
        rows = micro * total // LANES
        out = pl.pallas_call(
            functools.partial(relay_kernel, sizes),
            out_shape=jax.ShapeDtypeStruct((micro, toks, width), half),
            in_specs=[vmem] * 5 + [hbm] * 3,
            out_specs=vmem,
            scratch_shapes=[
                pltpu.VMEM((micro, toks, width), half),
                pltpu.VMEM((micro, n_node, cap, width), half),
                pltpu.VMEM((micro, n, cap, width), half),
                pltpu.VMEM((micro, n, cap, width), half),
                pltpu.VMEM((micro, n, cap, width), half),
                pltpu.VMEM((micro, toks, n_node * cap), half),
                pltpu.VMEM((n, rows, LANES), full),
                pltpu.VMEM((n, rows, LANES), full),
                pltpu.VMEM((micro, limit, total), half),
                pltpu.VMEM((micro, limit, 1), full),
                pltpu.VMEM((limit, width), full),
                pltpu.VMEM((FF_CHUNKS, width, chunk), half),
                pltpu.VMEM((FF_CHUNKS, width, chunk), half),
                pltpu.VMEM((FF_CHUNKS, chunk, width), half),
                dma((3, FF_CHUNKS)),
                dma((n,)), dma((n,)),
                dma((micro, n)), dma((micro, n)),
                dma((micro, n)), dma((micro, n)),
                dma((micro,)), dma((micro,)),
            ],
            compiler_params=pltpu.CompilerParams(collective_id=0, has_side_effects=True),
        )(
            tokens, expert_ids[0], slots[0], gates[0], gain,
            w_gate[0, 0], w_up[0, 0], w_down[0, 0],
        )
        return out[None]

    placed = (
        P(None, ("node", "local"), None),
        P("section", None, ("node", "local"), None),
        P("section", None, ("node", "local"), None),
        P("section", None, ("node", "local"), None),
        P("section", None),
        P("section", ("node", "local"), None, None),
        P("section", ("node", "local"), None, None),
        P("section", ("node", "local"), None, None),
    )
    return jax.shard_map(
        on_device,
        mesh=mesh,
        in_specs=placed,
        out_specs=P("section", None, ("node", "local"), None),
        check_vma=False,
    )
```

```python
import functools

import jax
import jax.numpy as jnp
from jax import lax
from jax.experimental import pallas as pl
from jax.experimental.pallas import tpu as pltpu
from jax.sharding import PartitionSpec as P

MESH = pl.DeviceIdType.MESH
LANES = 128
FF_CHUNKS = 3


def relay_kernel(
    sizes,
    tok_ref, ids_ref, slots_ref, gates_ref, gain_ref, wg_hbm, wu_hbm, wd_hbm,
    out_ref,
    held, packed, arrived, answer, parts, summed, back, hits, hits_t, meta_out, meta_in,
    pick, pick_t, pick_w, acc, wg, wu, wd,
    w_sem, meta_send, meta_recv, out_send, out_recv, fan_send, fan_recv,
    part_send, part_recv, back_send, back_recv, relay_send, relay_recv,
):
    n_sec, n_node, n_local, micro, toks, width, cap, limit = sizes
    n = n_node * n_local
    total = n * cap
    groups = total // LANES
    sec = lax.axis_index("section")
    node = lax.axis_index("node")
    local = lax.axis_index("local")
    me = node * n_local + local

    def device(p):
        return {"node": lax.div(p, n_local), "local": lax.rem(p, n_local)}

    def peers(body):
        lax.fori_loop(1, n, lambda i, c: (body(lax.rem(me + i, n)), c)[1], 0)

    barrier = pltpu.get_barrier_semaphore()
    peers(lambda p: pl.semaphore_signal(barrier, inc=1, device_id=device(p), device_id_type=MESH))
    for i in range(1, n_sec):
        pl.semaphore_signal(
            barrier, inc=1, device_id={"section": lax.rem(sec + i, n_sec)}, device_id_type=MESH
        )

    def weight_copies(c):
        chunk = wg.shape[2]
        cols = pl.ds(pl.multiple_of(c * chunk, chunk), chunk)
        return (
            pltpu.make_async_copy(wg_hbm.at[:, cols], wg.at[c], w_sem.at[0, c]),
            pltpu.make_async_copy(wu_hbm.at[:, cols], wu.at[c], w_sem.at[1, c]),
            pltpu.make_async_copy(wd_hbm.at[cols, :], wd.at[c], w_sem.at[2, c]),
        )

    for c in range(FF_CHUNKS):
        for copy in weight_copies(c):
            copy.start()

    def meta_copy(p):
        return pltpu.make_async_remote_copy(
            meta_out.at[p], meta_in.at[me], meta_send.at[p], meta_recv.at[me],
            device_id=device(p), device_id_type=MESH,
        )

    def out_copy(mb, j):
        return pltpu.make_async_remote_copy(
            packed.at[mb, j], arrived.at[mb, me], out_send.at[mb, j],
            out_recv.at[mb, me], device_id={"node": j}, device_id_type=MESH,
        )

    def fan_copy(mb, j, i):
        block = j * n_local + local
        return pltpu.make_async_remote_copy(
            arrived.at[mb, block], arrived.at[mb, block], fan_send.at[mb, j * n_local + i],
            fan_recv.at[mb, block], device_id={"local": i}, device_id_type=MESH,
        )

    def part_copy(mb, j, i):
        return pltpu.make_async_remote_copy(
            answer.at[mb, j * n_local + i], parts.at[mb, j * n_local + local],
            part_send.at[mb, j * n_local + i], part_recv.at[mb, j * n_local + local],
            device_id={"local": i}, device_id_type=MESH,
        )

    def back_copy(mb, j):
        return pltpu.make_async_remote_copy(
            summed.at[mb, j], back.at[mb, node], back_send.at[mb, j],
            back_recv.at[mb, node], device_id={"node": j}, device_id_type=MESH,
        )

    def nodes(body):
        lax.fori_loop(1, n_node, lambda i, c: (body(lax.rem(node + i, n_node)), c)[1], 0)

    def locals_(body):
        for i in range(1, n_local):
            body(lax.rem(local + i, n_local))

    def arrival(buffer, sem, p):
        return pltpu.make_async_remote_copy(
            buffer.at[p], buffer.at[p], sem.at[p], sem.at[p],
            device_id={"section": lax.rem(sec + 1, n_sec)}, device_id_type=MESH,
        )

    def relay_copy(mb):
        return pltpu.make_async_remote_copy(
            out_ref.at[mb], held.at[mb], relay_send.at[mb], relay_recv.at[mb],
            device_id={"section": lax.rem(sec + 1, n_sec)}, device_id_type=MESH,
        )

    slot_span = lax.broadcasted_iota(jnp.int32, (n_node * cap, toks), 0)
    exp_span = lax.broadcasted_iota(jnp.int32, (n, toks), 0)
    lane_span = lax.broadcasted_iota(jnp.int32, (LANES, toks), 0)
    row_span = lax.broadcasted_iota(jnp.int32, (n, micro * groups, LANES), 1)
    my_group = lax.div(me * cap, LANES)
    my_lane = lax.rem(me * cap, LANES)
    meta = jnp.zeros((n, micro * groups, LANES), jnp.float32)
    for mb in range(micro):
        hit = None
        weights = None
        for k in range(2):
            e = ids_ref[mb, k : k + 1, :]
            s = slots_ref[mb, k : k + 1, :]
            g = gates_ref[mb, k : k + 1, :]
            pos = jnp.where(s >= 0, lax.div(e, jnp.full_like(e, n_local)) * cap + s, -1)
            this = jnp.where(pos == slot_span, 1.0, 0.0)
            hit = this if hit is None else jnp.maximum(hit, this)
            lane = jnp.where(s >= 0, my_lane + s, -1)
            part = lax.dot_general(
                jnp.where(e == exp_span, g, 0.0),
                jnp.where(lane == lane_span, 1.0, 0.0),
                (((1,), (1,)), ((), ())),
                precision=lax.Precision.HIGHEST,
                preferred_element_type=jnp.float32,
            )
            weights = part if weights is None else weights + part
        hits[mb] = hit.astype(jnp.bfloat16)
        hits_t[mb] = hit.T.astype(jnp.bfloat16)
        meta = meta + jnp.where(row_span == mb * groups + my_group, weights[:, None, :], 0.0)
    meta_out[...] = meta
    meta_in[me] = meta_out[me]

    def pack(mb, h):
        floats = h.astype(jnp.float32)
        mean_square = jnp.mean(floats * floats, axis=-1, keepdims=True)
        normed = (floats * lax.rsqrt(mean_square + 1e-05) * gain_ref[...]).astype(jnp.bfloat16)
        rows = jnp.dot(hits[mb], normed, preferred_element_type=jnp.float32)
        for j in range(n_node):
            packed[mb, j] = rows[j * cap : (j + 1) * cap].astype(jnp.bfloat16)
        arrived[mb, me] = packed[mb, node]

    def dispatch(mb):
        nodes(lambda j: out_copy(mb, j).start())
        locals_(lambda i: fan_copy(mb, node, i).start())

    def hand_on(mb):
        def step(i, carry):
            j = lax.rem(node + n_node - i, n_node)
            arrival(arrived.at[mb], out_recv.at[mb], j * n_local + local).wait_recv()
            locals_(lambda k: fan_copy(mb, j, k).start())
            return carry

        lax.fori_loop(1, n_node, step, 0)

    @pl.when(sec == 0)
    def _():
        held[...] = tok_ref[...]
        pack(0, held[0])

    pl.semaphore_wait(barrier, n - 1 + n_sec - 1)
    peers(lambda p: meta_copy(p).start())

    @pl.when(sec == 0)
    def _():
        dispatch(0)
        for mb in range(1, micro):
            pack(mb, held[mb])
            dispatch(mb)
        for mb in range(micro):
            hand_on(mb)

    peers(lambda p: arrival(meta_in, meta_recv, p).wait_recv())
    meta = jnp.sum(meta_in[...], axis=0)
    upto = lax.broadcasted_iota(jnp.int32, (total, total), 0) <= lax.broadcasted_iota(
        jnp.int32, (total, total), 1
    )
    upto = jnp.where(upto, 1.0, 0.0).astype(jnp.bfloat16)
    spot = lax.broadcasted_iota(jnp.int32, (limit, total), 0).astype(jnp.float32)
    for mb in range(micro):
        w_row = jnp.concatenate(
            [meta[mb * groups + g : mb * groups + g + 1] for g in range(groups)], axis=1
        )
        w_rows = jnp.broadcast_to(w_row, (8, total))
        chosen = jnp.where(w_rows > 0.0, 1.0, 0.0)
        rank = jnp.dot(chosen.astype(jnp.bfloat16), upto, preferred_element_type=jnp.float32)
        rank = jnp.where(w_rows > 0.0, rank - 1.0, -1.0)
        is_at = spot == jnp.broadcast_to(rank[0:1], (limit, total))
        place = jnp.where(is_at, 1.0, 0.0)
        pick[mb] = place.astype(jnp.bfloat16)
        pick_t[mb] = place.T.astype(jnp.bfloat16)
        pick_w[mb] = jnp.sum(
            jnp.where(is_at, jnp.broadcast_to(w_row, (limit, total)), 0.0), axis=1, keepdims=True
        )

    @pl.when(sec > 0)
    def _():
        for mb in range(micro):
            relay_copy(mb).wait_recv()
            pack(mb, held[mb])
            dispatch(mb)
            hand_on(mb)

    def flat(blocks):
        if cap % 16:
            return blocks.astype(jnp.float32).reshape(-1, width).astype(jnp.bfloat16)
        return blocks.reshape(-1, width)

    for mb in range(micro):

        def wait_fan(j, carry):
            locals_(
                lambda i: arrival(arrived.at[mb], fan_recv.at[mb], j * n_local + i).wait_recv()
            )
            return carry

        lax.fori_loop(0, n_node, wait_fan, 0)
        rows = flat(arrived[mb])
        x = jnp.dot(pick[mb], rows, preferred_element_type=jnp.float32).astype(jnp.bfloat16)
        acc[...] = jnp.zeros_like(acc)

        def chunk_step(c, carry):
            if mb == 0:
                for copy in weight_copies(c):
                    copy.wait()
            gate = jnp.dot(x, wg[c], preferred_element_type=jnp.float32)
            up = jnp.dot(x, wu[c], preferred_element_type=jnp.float32)
            inner = (jax.nn.gelu(gate, approximate=True) * up).astype(jnp.bfloat16)
            acc[...] += jnp.dot(inner, wd[c], preferred_element_type=jnp.float32)
            return carry

        lax.fori_loop(0, FF_CHUNKS, chunk_step, 0)
        scaled = (pick_w[mb] * acc[...]).astype(jnp.bfloat16)
        spread = jnp.dot(pick_t[mb], scaled, preferred_element_type=jnp.float32)
        answer[mb] = spread.reshape(n, cap, width).astype(jnp.bfloat16)
        nodes(lambda j: locals_(lambda i: part_copy(mb, j, i).start()))
        locals_(lambda i: part_copy(mb, node, i).start())

    for mb in range(micro):

        def add_up(j):
            rows = answer[mb, j * n_local + local].astype(jnp.float32)
            locals_(
                lambda i: arrival(parts.at[mb], part_recv.at[mb], j * n_local + i).wait_recv()
            )
            for i in range(1, n_local):
                block = j * n_local + lax.rem(local + i, n_local)
                rows = rows + parts[mb, block].astype(jnp.float32)
            return rows.astype(jnp.bfloat16)

        def send_back(j):
            summed[mb, j] = add_up(j)
            back_copy(mb, j).start()

        nodes(send_back)
        back[mb, node] = add_up(node)
        nodes(lambda j: arrival(back.at[mb], back_recv.at[mb], j).wait_recv())
        mixed = jnp.dot(hits_t[mb], flat(back[mb]), preferred_element_type=jnp.float32)
        out_ref[mb] = (held[mb].astype(jnp.float32) + mixed).astype(jnp.bfloat16)

        @pl.when(sec < n_sec - 1)
        def _():
            relay_copy(mb).start()

    peers(lambda p: meta_copy(p).wait_send())
    for mb in range(micro):

        def settle(j):
            locals_(lambda i: fan_copy(mb, j, i).wait_send())
            locals_(lambda i: part_copy(mb, j, i).wait_send())

        nodes(lambda j: (out_copy(mb, j).wait_send(), back_copy(mb, j).wait_send()))
        nodes(settle)
        settle(node)

    @pl.when(sec < n_sec - 1)
    def _():
        for mb in range(micro):
            relay_copy(mb).wait_send()


def solution(mesh):
    n_sec, n_node, n_local = mesh.shape["section"], mesh.shape["node"], mesh.shape["local"]
    n = n_node * n_local

    def on_device(tokens, expert_ids, slots, gates, gain, w_gate, w_up, w_down):
        micro, toks, width = tokens.shape
        hidden = w_gate.shape[3]
        cap = 2 * toks // n_node
        limit = 4 * toks
        total = n * cap
        chunk = hidden // FF_CHUNKS
        sizes = (n_sec, n_node, n_local, micro, toks, width, cap, limit)
        half, full = jnp.bfloat16, jnp.float32
        vmem = pl.BlockSpec(memory_space=pltpu.VMEM)
        hbm = pl.BlockSpec(memory_space=pl.ANY)
        dma = pltpu.SemaphoreType.DMA
        rows = micro * total // LANES
        out = pl.pallas_call(
            functools.partial(relay_kernel, sizes),
            out_shape=jax.ShapeDtypeStruct((micro, toks, width), half),
            in_specs=[vmem] * 5 + [hbm] * 3,
            out_specs=vmem,
            scratch_shapes=[
                pltpu.VMEM((micro, toks, width), half),
                pltpu.VMEM((micro, n_node, cap, width), half),
                pltpu.VMEM((micro, n, cap, width), half),
                pltpu.VMEM((micro, n, cap, width), half),
                pltpu.VMEM((micro, n, cap, width), half),
                pltpu.VMEM((micro, n_node, cap, width), half),
                pltpu.VMEM((micro, n_node, cap, width), half),
                pltpu.VMEM((micro, n_node * cap, toks), half),
                pltpu.VMEM((micro, toks, n_node * cap), half),
                pltpu.VMEM((n, rows, LANES), full),
                pltpu.VMEM((n, rows, LANES), full),
                pltpu.VMEM((micro, limit, total), half),
                pltpu.VMEM((micro, total, limit), half),
                pltpu.VMEM((micro, limit, 1), full),
                pltpu.VMEM((limit, width), full),
                pltpu.VMEM((FF_CHUNKS, width, chunk), half),
                pltpu.VMEM((FF_CHUNKS, width, chunk), half),
                pltpu.VMEM((FF_CHUNKS, chunk, width), half),
                dma((3, FF_CHUNKS)),
                dma((n,)), dma((n,)),
                dma((micro, n_node)), dma((micro, n)),
                dma((micro, n)), dma((micro, n)),
                dma((micro, n)), dma((micro, n)),
                dma((micro, n_node)), dma((micro, n_node)),
                dma((micro,)), dma((micro,)),
            ],
            compiler_params=pltpu.CompilerParams(collective_id=0, has_side_effects=True),
        )(
            tokens, *(jnp.swapaxes(a[0], 1, 2) for a in (expert_ids, slots, gates)), gain,
            w_gate[0, 0], w_up[0, 0], w_down[0, 0],
        )
        return out[None]

    placed = (
        P(None, ("node", "local"), None),
        P("section", None, ("node", "local"), None),
        P("section", None, ("node", "local"), None),
        P("section", None, ("node", "local"), None),
        P("section", None),
        P("section", ("node", "local"), None, None),
        P("section", ("node", "local"), None, None),
        P("section", ("node", "local"), None, None),
    )
    return jax.shard_map(
        on_device,
        mesh=mesh,
        in_specs=placed,
        out_specs=P("section", None, ("node", "local"), None),
        check_vma=False,
    )
```

```python
import functools

import jax
import jax.numpy as jnp
from jax import lax
from jax.experimental import pallas as pl
from jax.experimental.pallas import tpu as pltpu
from jax.sharding import PartitionSpec as P

MESH = pl.DeviceIdType.MESH
LANES = 128
FF_CHUNKS = 3


def relay_kernel(
    sizes,
    tok_ref, ids_ref, slots_ref, gates_ref, gain_ref, wg_hbm, wu_hbm, wd_hbm,
    out_ref,
    held, packed, arrived, answer, parts, summed, back, hits, hits_t, meta_out, meta_in,
    pick, pick_t, pick_w, acc, wg, wu, wd,
    w_sem, meta_send, meta_recv, out_send, out_recv, fan_send, fan_recv,
    part_send, part_recv, back_send, back_recv, relay_send, relay_recv,
):
    n_sec, n_node, n_local, micro, toks, width, cap, limit = sizes
    n = n_node * n_local
    total = n * cap
    groups = total // LANES
    sec = lax.axis_index("section")
    node = lax.axis_index("node")
    local = lax.axis_index("local")
    me = node * n_local + local

    def device(p):
        return {"node": lax.div(p, n_local), "local": lax.rem(p, n_local)}

    def peers(body):
        lax.fori_loop(1, n, lambda i, c: (body(lax.rem(me + i, n)), c)[1], 0)

    barrier = pltpu.get_barrier_semaphore()
    peers(lambda p: pl.semaphore_signal(barrier, inc=1, device_id=device(p), device_id_type=MESH))
    for i in range(1, n_sec):
        pl.semaphore_signal(
            barrier, inc=1, device_id={"section": lax.rem(sec + i, n_sec)}, device_id_type=MESH
        )

    def weight_copies(c):
        chunk = wg.shape[2]
        cols = pl.ds(pl.multiple_of(c * chunk, chunk), chunk)
        return (
            pltpu.make_async_copy(wg_hbm.at[:, cols], wg.at[c], w_sem.at[0, c]),
            pltpu.make_async_copy(wu_hbm.at[:, cols], wu.at[c], w_sem.at[1, c]),
            pltpu.make_async_copy(wd_hbm.at[cols, :], wd.at[c], w_sem.at[2, c]),
        )

    for c in range(FF_CHUNKS):
        for copy in weight_copies(c):
            copy.start()

    def meta_copy(p):
        return pltpu.make_async_remote_copy(
            meta_out.at[p], meta_in.at[me], meta_send.at[p], meta_recv.at[me],
            device_id=device(p), device_id_type=MESH,
        )

    def out_copy(mb, j):
        return pltpu.make_async_remote_copy(
            packed.at[mb, j], arrived.at[mb, me], out_send.at[mb, j],
            out_recv.at[mb, me], device_id={"node": j}, device_id_type=MESH,
        )

    def fan_copy(mb, j, i):
        block = j * n_local + local
        return pltpu.make_async_remote_copy(
            arrived.at[mb, block], arrived.at[mb, block], fan_send.at[mb, j * n_local + i],
            fan_recv.at[mb, block], device_id={"local": i}, device_id_type=MESH,
        )

    def part_copy(mb, j, i):
        return pltpu.make_async_remote_copy(
            answer.at[mb, j * n_local + i], parts.at[mb, j * n_local + local],
            part_send.at[mb, j * n_local + i], part_recv.at[mb, j * n_local + local],
            device_id={"local": i}, device_id_type=MESH,
        )

    def back_copy(mb, j):
        return pltpu.make_async_remote_copy(
            summed.at[mb, j], back.at[mb, node], back_send.at[mb, j],
            back_recv.at[mb, node], device_id={"node": j}, device_id_type=MESH,
        )

    upper = node >= n_node // 2
    from_end = jnp.where(upper, node, n_node - 1 - node)

    def nodes(body, near_first=False):
        def step(i, carry):
            place = n_node - 2 - i if near_first else i
            place = jnp.where(place >= from_end, place + 1, place)
            body(jnp.where(upper, place, n_node - 1 - place))
            return carry

        lax.fori_loop(0, n_node - 1, step, 0)

    def locals_(body):
        for i in range(1, n_local):
            body(lax.rem(local + i, n_local))

    def arrival(buffer, sem, p):
        return pltpu.make_async_remote_copy(
            buffer.at[p], buffer.at[p], sem.at[p], sem.at[p],
            device_id={"section": lax.rem(sec + 1, n_sec)}, device_id_type=MESH,
        )

    def relay_copy(mb):
        return pltpu.make_async_remote_copy(
            out_ref.at[mb], held.at[mb], relay_send.at[mb], relay_recv.at[mb],
            device_id={"section": lax.rem(sec + 1, n_sec)}, device_id_type=MESH,
        )

    slot_span = lax.broadcasted_iota(jnp.int32, (n_node * cap, toks), 0)
    exp_span = lax.broadcasted_iota(jnp.int32, (n, toks), 0)
    lane_span = lax.broadcasted_iota(jnp.int32, (LANES, toks), 0)
    row_span = lax.broadcasted_iota(jnp.int32, (n, micro * groups, LANES), 1)
    my_group = lax.div(me * cap, LANES)
    my_lane = lax.rem(me * cap, LANES)
    meta = jnp.zeros((n, micro * groups, LANES), jnp.float32)
    for mb in range(micro):
        hit = None
        weights = None
        for k in range(2):
            e = ids_ref[mb, k : k + 1, :]
            s = slots_ref[mb, k : k + 1, :]
            g = gates_ref[mb, k : k + 1, :]
            pos = jnp.where(s >= 0, lax.div(e, jnp.full_like(e, n_local)) * cap + s, -1)
            this = jnp.where(pos == slot_span, 1.0, 0.0)
            hit = this if hit is None else jnp.maximum(hit, this)
            lane = jnp.where(s >= 0, my_lane + s, -1)
            part = lax.dot_general(
                jnp.where(e == exp_span, g, 0.0),
                jnp.where(lane == lane_span, 1.0, 0.0),
                (((1,), (1,)), ((), ())),
                precision=lax.Precision.HIGHEST,
                preferred_element_type=jnp.float32,
            )
            weights = part if weights is None else weights + part
        hits[mb] = hit.astype(jnp.bfloat16)
        hits_t[mb] = hit.T.astype(jnp.bfloat16)
        meta = meta + jnp.where(row_span == mb * groups + my_group, weights[:, None, :], 0.0)
    meta_out[...] = meta
    meta_in[me] = meta_out[me]

    def pack(mb, h):
        floats = h.astype(jnp.float32)
        mean_square = jnp.mean(floats * floats, axis=-1, keepdims=True)
        normed = (floats * lax.rsqrt(mean_square + 1e-05) * gain_ref[...]).astype(jnp.bfloat16)
        rows = jnp.dot(hits[mb], normed, preferred_element_type=jnp.float32)
        for j in range(n_node):
            packed[mb, j] = rows[j * cap : (j + 1) * cap].astype(jnp.bfloat16)
        arrived[mb, me] = packed[mb, node]

    def dispatch(mb):
        nodes(lambda j: out_copy(mb, j).start())

    def hand_on(mb):
        locals_(lambda i: fan_copy(mb, node, i).start())

        def step(j):
            arrival(arrived.at[mb], out_recv.at[mb], j * n_local + local).wait_recv()
            locals_(lambda k: fan_copy(mb, j, k).start())

        nodes(step, near_first=True)

    @pl.when(sec == 0)
    def _():
        held[...] = tok_ref[...]
        pack(0, held[0])

    pl.semaphore_wait(barrier, n - 1 + n_sec - 1)
    peers(lambda p: meta_copy(p).start())

    @pl.when(sec == 0)
    def _():
        dispatch(0)
        for mb in range(1, micro):
            pack(mb, held[mb])
            dispatch(mb)
        for mb in range(micro):
            hand_on(mb)

    peers(lambda p: arrival(meta_in, meta_recv, p).wait_recv())
    meta = jnp.sum(meta_in[...], axis=0)
    upto = lax.broadcasted_iota(jnp.int32, (total, total), 0) <= lax.broadcasted_iota(
        jnp.int32, (total, total), 1
    )
    upto = jnp.where(upto, 1.0, 0.0).astype(jnp.bfloat16)
    spot = lax.broadcasted_iota(jnp.int32, (limit, total), 0).astype(jnp.float32)
    for mb in range(micro):
        w_row = jnp.concatenate(
            [meta[mb * groups + g : mb * groups + g + 1] for g in range(groups)], axis=1
        )
        w_rows = jnp.broadcast_to(w_row, (8, total))
        chosen = jnp.where(w_rows > 0.0, 1.0, 0.0)
        rank = jnp.dot(chosen.astype(jnp.bfloat16), upto, preferred_element_type=jnp.float32)
        rank = jnp.where(w_rows > 0.0, rank - 1.0, -1.0)
        is_at = spot == jnp.broadcast_to(rank[0:1], (limit, total))
        place = jnp.where(is_at, 1.0, 0.0)
        pick[mb] = place.astype(jnp.bfloat16)
        pick_t[mb] = place.T.astype(jnp.bfloat16)
        pick_w[mb] = jnp.sum(
            jnp.where(is_at, jnp.broadcast_to(w_row, (limit, total)), 0.0), axis=1, keepdims=True
        )

    @pl.when(sec > 0)
    def _():
        for mb in range(micro):
            relay_copy(mb).wait_recv()
            pack(mb, held[mb])
            dispatch(mb)
            if mb == 0:
                hand_on(mb)

    def flat(blocks):
        if cap % 16:
            return blocks.astype(jnp.float32).reshape(-1, width).astype(jnp.bfloat16)
        return blocks.reshape(-1, width)

    for mb in range(micro):

        def wait_fan(j, carry):
            locals_(
                lambda i: arrival(arrived.at[mb], fan_recv.at[mb], j * n_local + i).wait_recv()
            )
            return carry

        lax.fori_loop(0, n_node, wait_fan, 0)
        rows = flat(arrived[mb])
        x = jnp.dot(pick[mb], rows, preferred_element_type=jnp.float32).astype(jnp.bfloat16)
        acc[...] = jnp.zeros_like(acc)

        def chunk_step(c, carry):
            if mb == 0:
                for copy in weight_copies(c):
                    copy.wait()
            gate = jnp.dot(x, wg[c], preferred_element_type=jnp.float32)
            up = jnp.dot(x, wu[c], preferred_element_type=jnp.float32)
            inner = (jax.nn.gelu(gate, approximate=True) * up).astype(jnp.bfloat16)
            acc[...] += jnp.dot(inner, wd[c], preferred_element_type=jnp.float32)
            if mb == 0:

                @pl.when((sec > 0) & (c == 0))
                def _():
                    for later in range(1, micro):
                        hand_on(later)

            return carry

        lax.fori_loop(0, FF_CHUNKS, chunk_step, 0)
        scaled = (pick_w[mb] * acc[...]).astype(jnp.bfloat16)
        spread = jnp.dot(pick_t[mb], scaled, preferred_element_type=jnp.float32)
        answer[mb] = spread.reshape(n, cap, width).astype(jnp.bfloat16)
        nodes(lambda j: locals_(lambda i: part_copy(mb, j, i).start()))
        locals_(lambda i: part_copy(mb, node, i).start())

    for mb in range(micro):

        def add_up(j):
            rows = answer[mb, j * n_local + local].astype(jnp.float32)
            locals_(
                lambda i: arrival(parts.at[mb], part_recv.at[mb], j * n_local + i).wait_recv()
            )
            for i in range(1, n_local):
                block = j * n_local + lax.rem(local + i, n_local)
                rows = rows + parts[mb, block].astype(jnp.float32)
            return rows.astype(jnp.bfloat16)

        def send_back(j):
            summed[mb, j] = add_up(j)
            back_copy(mb, j).start()

        nodes(send_back)
        back[mb, node] = add_up(node)

    for mb in range(micro):
        nodes(lambda j: arrival(back.at[mb], back_recv.at[mb], j).wait_recv())
        mixed = jnp.dot(hits_t[mb], flat(back[mb]), preferred_element_type=jnp.float32)
        out_ref[mb] = (held[mb].astype(jnp.float32) + mixed).astype(jnp.bfloat16)

        @pl.when(sec < n_sec - 1)
        def _():
            relay_copy(mb).start()

    peers(lambda p: meta_copy(p).wait_send())
    for mb in range(micro):

        def settle(j):
            locals_(lambda i: fan_copy(mb, j, i).wait_send())
            locals_(lambda i: part_copy(mb, j, i).wait_send())

        nodes(lambda j: (out_copy(mb, j).wait_send(), back_copy(mb, j).wait_send()))
        nodes(settle)
        settle(node)

    @pl.when(sec < n_sec - 1)
    def _():
        for mb in range(micro):
            relay_copy(mb).wait_send()


def solution(mesh):
    n_sec, n_node, n_local = mesh.shape["section"], mesh.shape["node"], mesh.shape["local"]
    n = n_node * n_local

    def on_device(tokens, expert_ids, slots, gates, gain, w_gate, w_up, w_down):
        micro, toks, width = tokens.shape
        hidden = w_gate.shape[3]
        cap = 2 * toks // n_node
        limit = 4 * toks
        total = n * cap
        chunk = hidden // FF_CHUNKS
        sizes = (n_sec, n_node, n_local, micro, toks, width, cap, limit)
        half, full = jnp.bfloat16, jnp.float32
        vmem = pl.BlockSpec(memory_space=pltpu.VMEM)
        hbm = pl.BlockSpec(memory_space=pl.ANY)
        dma = pltpu.SemaphoreType.DMA
        rows = micro * total // LANES
        out = pl.pallas_call(
            functools.partial(relay_kernel, sizes),
            out_shape=jax.ShapeDtypeStruct((micro, toks, width), half),
            in_specs=[vmem] * 5 + [hbm] * 3,
            out_specs=vmem,
            scratch_shapes=[
                pltpu.VMEM((micro, toks, width), half),
                pltpu.VMEM((micro, n_node, cap, width), half),
                pltpu.VMEM((micro, n, cap, width), half),
                pltpu.VMEM((micro, n, cap, width), half),
                pltpu.VMEM((micro, n, cap, width), half),
                pltpu.VMEM((micro, n_node, cap, width), half),
                pltpu.VMEM((micro, n_node, cap, width), half),
                pltpu.VMEM((micro, n_node * cap, toks), half),
                pltpu.VMEM((micro, toks, n_node * cap), half),
                pltpu.VMEM((n, rows, LANES), full),
                pltpu.VMEM((n, rows, LANES), full),
                pltpu.VMEM((micro, limit, total), half),
                pltpu.VMEM((micro, total, limit), half),
                pltpu.VMEM((micro, limit, 1), full),
                pltpu.VMEM((limit, width), full),
                pltpu.VMEM((FF_CHUNKS, width, chunk), half),
                pltpu.VMEM((FF_CHUNKS, width, chunk), half),
                pltpu.VMEM((FF_CHUNKS, chunk, width), half),
                dma((3, FF_CHUNKS)),
                dma((n,)), dma((n,)),
                dma((micro, n_node)), dma((micro, n)),
                dma((micro, n)), dma((micro, n)),
                dma((micro, n)), dma((micro, n)),
                dma((micro, n_node)), dma((micro, n_node)),
                dma((micro,)), dma((micro,)),
            ],
            compiler_params=pltpu.CompilerParams(collective_id=0, has_side_effects=True),
        )(
            tokens, *(jnp.swapaxes(a[0], 1, 2) for a in (expert_ids, slots, gates)), gain,
            w_gate[0, 0], w_up[0, 0], w_down[0, 0],
        )
        return out[None]

    placed = (
        P(None, ("node", "local"), None),
        P("section", None, ("node", "local"), None),
        P("section", None, ("node", "local"), None),
        P("section", None, ("node", "local"), None),
        P("section", None),
        P("section", ("node", "local"), None, None),
        P("section", ("node", "local"), None, None),
        P("section", ("node", "local"), None, None),
    )
    return jax.shard_map(
        on_device,
        mesh=mesh,
        in_specs=placed,
        out_specs=P("section", None, ("node", "local"), None),
        check_vma=False,
    )
```
